32 devices in a mesh: dp: 2 (over z, core), sp: 16 (over x, y).
Axes of the slice: x: 4, y: 4, z: 1, core: 2. Of those that a mesh axis runs over, the one named last changes fastest.
The devices are a block of a 4x4x8 slice.
Arguments:
- x: bfloat16 [4096, 4096], P(('dp', 'sp')), parts along dimension 0
- gain: bfloat16 [4096], replicated
- wq: bfloat16 [4096, 12288], replicated
- wk: bfloat16 [4096, 1024], replicated
- wv: bfloat16 [4096, 1024], replicated
- wo: bfloat16 [12288, 4096], replicated
Outputs:
- output: bfloat16 [4096, 4096], P(('dp', 'sp')), parts along dimension 0
There are 2 independent parts. The reference program is written for one: setup_inputs(seed, part) draws one part's arguments, and reference() takes and returns one part's arrays. A program takes and returns all parts, laid end to end along the dimension named above; an argument that names none is the same for every part.
All inputs are finite; a program needn't handle non-finite values.
Results may differ from the reference program's by a relative error of at most 0.012.
Values are sent between devices in bfloat16 or wider.
A program may use at most 768 MiB of HBM per device.

```python
import jax
import jax.numpy as jnp
from jax import lax

ROWS = 2048
D = 4096
HEADS = 96
KV_HEADS = 8
HEAD = 128
THETA = 10000


def setup_inputs(seed: int = 0, part: int = 0) -> dict:
    kx, kn, kq, kk, kv, ko = jax.random.split(jax.random.key(seed), 6)

    def weights(key, rows, columns):
        return jax.random.normal(key, (rows, columns), jnp.float32) * rows**-0.5

    drawn = {
        "x": jax.random.normal(jax.random.fold_in(kx, part), (ROWS, D), jnp.float32),
        "gain": 1 + 0.1 * jax.random.normal(kn, (D,), jnp.float32),
        "wq": 2 * weights(kq, D, HEADS * HEAD),
        "wk": 2 * weights(kk, D, KV_HEADS * HEAD),
        "wv": 4 * weights(kv, D, KV_HEADS * HEAD),
        "wo": weights(ko, HEADS * HEAD, D),
    }
    return {k: v.astype(jnp.bfloat16) for k, v in drawn.items()}


def normed(x, gain):
    wide = x.astype(jnp.float32)
    scale = lax.rsqrt(jnp.mean(wide * wide, -1, keepdims=True) + 1e-6)
    return (wide * scale * gain.astype(jnp.float32)).astype(jnp.bfloat16)


def turned(t, place, theta):
    half = t.shape[-1] // 2
    angle = place.astype(jnp.float32)[:, None] * theta ** (-jnp.arange(half, dtype=jnp.float32) / half)
    cos, sin = jnp.cos(angle)[:, None], jnp.sin(angle)[:, None]
    a, b = t[..., :half].astype(jnp.float32), t[..., half:].astype(jnp.float32)
    return jnp.concatenate([a * cos - b * sin, b * cos + a * sin], -1).astype(jnp.bfloat16)


def matmul(a, w):
    return jnp.dot(a, w, preferred_element_type=jnp.float32).astype(jnp.bfloat16)


def einsum(form, a, b):
    return jnp.einsum(form, a.astype(jnp.float32), b.astype(jnp.float32))


def attention(q, k, v):
    scores = einsum("tgsd,ugd->gstu", q, k) * q.shape[-1] ** -0.5
    token = jnp.arange(q.shape[0])
    scores = jnp.where(token[:, None] >= token, scores, -jnp.inf)
    weights = jax.nn.softmax(scores, -1).astype(jnp.bfloat16)
    return einsum("gstu,ugd->tgsd", weights, v).astype(jnp.bfloat16)


def reference(x, gain, wq, wk, wv, wo):
    a, place = normed(x, gain), jnp.arange(ROWS)
    q = turned(matmul(a, wq).reshape(ROWS, HEADS, HEAD), place, THETA).reshape(ROWS, KV_HEADS, -1, HEAD)
    k = turned(matmul(a, wk).reshape(ROWS, KV_HEADS, HEAD), place, THETA)
    v = matmul(a, wv).reshape(ROWS, KV_HEADS, HEAD)
    seen = attention(q, k, v).reshape(ROWS, HEADS * HEAD)
    return (x.astype(jnp.float32) + jnp.dot(seen, wo, preferred_element_type=jnp.float32)).astype(jnp.bfloat16)
```

```python
import functools
import math

import jax
import jax.numpy as jnp
from jax import lax
from jax.experimental import pallas as pl
from jax.experimental.pallas import tpu as pltpu
from jax.sharding import PartitionSpec as P

HEAD = 128
THETA = 10000
LOG2E = 1.4426950408889634
HIDDEN = -2e30
FAR = 1e30
WIDE = 512
SLOTS = 9
STRIP = 2


def _dot(a, b, ca=1, cb=0):
    return lax.dot_general(a, b, (((ca,), (cb,)), ((), ())), preferred_element_type=jnp.float32)


def _kernel(side, x_ref, gain_ref, cos_ref, sin_ref, wq_ref, wk_ref, wv_ref, wo_ref, y_ref,
            a_s, kv_s, q_s, o_s, acc_s, ring, s0, s1, ring_sem, send_sem, recv_sem):
    own, depth = x_ref.shape
    heads, kvh = q_s.shape[0], kv_s.shape[0]
    group = heads // kvh
    pairs = kvh // 2
    n = side * side
    nq = heads * HEAD // WIDE
    per_q = WIDE // HEAD
    no = depth // WIDE
    rows_o = 2 * group * HEAD
    me = lax.axis_index("sp")
    mx, my = lax.div(me, side), lax.rem(me, side)

    per_pair = nq // pairs
    q_end = [min(nq, per_pair * (p + 1) + LEAD) for p in range(pairs)]
    q_end[-1] = nq
    q_start = [0] + q_end[:-1]

    def pick(table, p):
        got = jnp.int32(table[-1])
        for i in range(len(table) - 2, -1, -1):
            got = jnp.where(p == i, table[i], got)
        return got

    chunks = pairs + nq + pairs * no

    def issue(t):
        s = lax.rem(t, SLOTS)
        at = pairs

        def kv(p):
            cols = pl.ds(pl.multiple_of(p * (WIDE // 2), WIDE // 2), WIDE // 2)
            pltpu.make_async_copy(wk_ref.at[:, cols], ring.at[s, :, 0 : WIDE // 2], ring_sem.at[s]).start()
            pltpu.make_async_copy(wv_ref.at[:, cols], ring.at[s, :, WIDE // 2 :], ring_sem.at[s]).start()

        def q(c):
            pltpu.make_async_copy(wq_ref.at[:, pl.ds(pl.multiple_of(c * WIDE, WIDE), WIDE)], ring.at[s], ring_sem.at[s]).start()

        def o(p, c):
            pltpu.make_async_copy(
                wo_ref.at[pl.ds(pl.multiple_of(p * rows_o, rows_o), rows_o), pl.ds(pl.multiple_of(c * WIDE, WIDE), WIDE)],
                ring.at[s, 0:rows_o, :], ring_sem.at[s]).start()

        if isinstance(t, int) and t < pairs:
            kv(t)
            return
        is_q, is_o, qi, oi, op = False, False, jnp.int32(0), jnp.int32(0), jnp.int32(0)
        for p in range(pairs):
            nqp = q_end[p] - q_start[p]
            inq = (t >= at) & (t < at + nqp)
            ino = (t >= at + nqp) & (t < at + nqp + no)
            qi = jnp.where(inq, q_start[p] + t - at, qi)
            oi = jnp.where(ino, t - at - nqp, oi)
            op = jnp.where(ino, p, op)
            is_q = is_q | inq
            is_o = is_o | ino
            at += nqp + no

        @pl.when(is_q)
        def _():
            q(qi)

        @pl.when(is_o)
        def _():
            o(op, oi)

    def landed(t, rows):
        s = lax.rem(t, SLOTS)
        ref = ring.at[s, 0:rows, :]
        pltpu.make_async_copy(ref, ref, ring_sem.at[s]).wait()
        return s

    def place(j):
        return (mx, my) if j == 0 else (my, mx)

    def device(j, g, b):
        return g * side + b if j == 0 else b * side + g

    def step(v, d):
        return lax.rem(v + d + side, side)

    def copy(ref, h, i, peer):
        return pltpu.make_async_remote_copy(src_ref=ref, dst_ref=ref, send_sem=send_sem.at[h, i], recv_sem=recv_sem.at[h, i],
                                            device_id={"sp": peer}, device_id_type=pl.DeviceIdType.MESH)

    def transfers(p, j):
        h = 2 * p + j
        g, b = place(j)
        right1, left1 = device(j, g, step(b, 1)), device(j, g, step(b, -1))
        right2, left2 = device(j, step(g, 1), b), device(j, step(g, -1), b)
        blk = lambda d, kind: kv_s.at[h, g, kind, step(b, d)]
        both = lambda d: kv_s.at[h, g, :, step(b, d)]
        grp = lambda d: kv_s.at[h, step(g, d)]
        half = lambda d, kind: kv_s.at[h, step(g, d), kind]
        sent = [(both(0), right1), (both(0), left1), (blk(-1, 0), right1), (blk(1, 1), left1),
                (grp(0), right2), (grp(0), left2), (half(-1, 0), right2), (half(1, 1), left2)]
        come = [both(-1), both(1), blk(-2, 0), blk(2, 1), grp(-1), grp(1), half(-2, 0), half(2, 1)]
        return h, sent, come

    def event(p, waits, starts):
        for j in (0, 1):
            h, sent, come = transfers(p, j)
            for i in waits:
                copy(come[i], h, i, me).wait_recv()
            for i in starts:
                copy(sent[i][0], h, i, sent[i][1]).start()

    events = [((), (0, 1)), ((0, 1), (2, 3)), ((2, 3), (4, 5)), ((4, 5), (6, 7)), ((6, 7), ())]

    for t in range(min(SLOTS, chunks)):
        issue(t)

    barrier = pltpu.get_barrier_semaphore()
    around = [device(0, mx, step(my, 1)), device(0, mx, step(my, -1)), device(0, step(mx, 1), my), device(0, step(mx, -1), my)]
    for peer in around:
        pl.semaphore_signal(barrier, inc=1, device_id={"sp": peer}, device_id_type=pl.DeviceIdType.MESH)

    gain = gain_ref[...].astype(jnp.float32)

    def norm(i, _):
        rows = pl.ds(pl.multiple_of(i * 16, 16), 16)
        wide = x_ref[rows, :].astype(jnp.float32)
        scale = lax.rsqrt(jnp.mean(wide * wide, -1, keepdims=True) + 1e-6)
        a_s[rows, :] = (wide * scale * gain).astype(jnp.bfloat16)
        for c in range(no):
            acc_s[c, rows, :] = wide[:, c * WIDE : (c + 1) * WIDE]

    lax.fori_loop(0, own // 16, norm, None)
    pl.semaphore_wait(barrier, len(around))

    def turned(t):
        wide = t.astype(jnp.bfloat16).astype(jnp.float32)
        return (wide * cos_ref[...] + pltpu.roll(wide, HEAD // 2, 1) * sin_ref[...]).astype(jnp.bfloat16)

    def kv_chunk(p, _):
        s = landed(p, depth)
        got = _dot(a_s[...], ring[s])
        issue(p + SLOTS)
        for j in (0, 1):
            g, b = place(j)
            k = turned(got[:, j * HEAD : (j + 1) * HEAD])
            v = got[:, WIDE // 2 + j * HEAD : WIDE // 2 + (j + 1) * HEAD]
            kv_s[2 * p + j, g, 0, b] = k
            kv_s[2 * p + j, g, 1, b] = v.T.astype(jnp.bfloat16)

        @pl.when(p == 1)
        def _():
            event(0, *events[0])

    lax.fori_loop(0, pairs, kv_chunk, None)

    def q_chunk(c, t):
        s = landed(t, depth)
        got = _dot(a_s[...], ring[s])
        issue(t + SLOTS)
        for i in range(per_q):
            q_s[c * per_q + i] = turned(got[:, i * HEAD : (i + 1) * HEAD])
        for at, p, e in Q_EVENTS:

            @pl.when(c == at)
            def _():
                event(p, *events[e])

        return t + 1

    e = HEAD**-0.5 * LOG2E
    cols = STRIP * own
    shown = lax.broadcasted_iota(jnp.int32, (own, cols), 0) <= lax.rem(lax.broadcasted_iota(jnp.int32, (own, cols), 1), own)
    ones = jnp.ones((16, n * own), jnp.bfloat16)

    def attend(p, j):
        h = 2 * p + j
        even = j == 0
        g, b = jnp.where(even, mx, my), jnp.where(even, my, mx)
        blocks, hides = [], []
        for i in range(n):
            at = lax.rem(g * side + b + i, n)
            gi, bi = lax.div(at, side), lax.rem(at, side)
            blocks.append((gi, bi))
            hides.append(None if i == 0 else jnp.where(jnp.where(even, at, bi * side + gi) < me, 0.0, FAR))
        keys = jnp.concatenate([kv_s[h, gi, 0, bi] for gi, bi in blocks], axis=0)
        values = jnp.concatenate([jnp.concatenate([kv_s[h, gi, 1, bi] for gi, bi in blocks], axis=1), ones], axis=0)
        scores = (s0, s1)

        def score(i):
            q = jnp.concatenate([q_s[h * group + i * STRIP + r] for r in range(STRIP)], axis=0)
            scores[i % 2][...] = _dot(keys, q, 1, 1)

        def mix(i):
            s_ref = scores[i % 2]
            top = None
            for r in range(n):
                s = s_ref[r * own : (r + 1) * own, :]
                if r == 0:
                    s = jnp.where(shown, s, HIDDEN)
                part = s.reshape(own // 8, 8, cols).max(axis=0)
                if r:
                    part = part - hides[r]
                top = part if top is None else jnp.maximum(top, part)
            top = top.max(axis=0, keepdims=True)
            weights = []
            for r in range(n):
                s = s_ref[r * own : (r + 1) * own, :]
                if r == 0:
                    s = jnp.where(shown, s, HIDDEN)
                weights.append(jnp.exp2((s - (top if r == 0 else top + hides[r])) * e).astype(jnp.bfloat16))
            got = _dot(values, jnp.concatenate(weights, axis=0))
            out = (got[:HEAD] * (1 / got[HEAD : HEAD + 1])).T.astype(jnp.bfloat16)
            for r in range(STRIP):
                o_s[j * group + i * STRIP + r] = out[r * own : (r + 1) * own, :]

        strips = group // STRIP
        score(0)
        for i in range(strips):
            if i + 1 < strips:
                score(i + 1)
            mix(i)

    def o_chunk(c, t):
        s = landed(t, rows_o)
        seen = jnp.concatenate([o_s[i] for i in range(2 * group)], axis=1)
        acc_s[c] += _dot(seen, ring[s, 0:rows_o, :])
        issue(t + SLOTS)
        return t + 1

    def stage(p, t):
        t = lax.fori_loop(pick(q_start, p), pick(q_end, p), q_chunk, t)

        def head(j, _):
            for at, ep, ee in A_EVENTS:

                @pl.when(2 * p + j == at)
                def _():
                    event(ep, *events[ee])

            attend(p, j)

        lax.fori_loop(0, 2, head, None)
        return lax.fori_loop(0, no, o_chunk, t)

    lax.fori_loop(0, pairs, stage, jnp.int32(pairs))
    for c in range(no):
        y_ref[:, c * WIDE : (c + 1) * WIDE] = acc_s[c].astype(jnp.bfloat16)
    for p in range(pairs):
        for j in (0, 1):
            h, sent, _ = transfers(p, j)
            for i, (ref, peer) in enumerate(sent):
                copy(ref, h, i, peer).wait_send()


LEAD = 10
Q_EVENTS = ((0, 0, 1), (0, 1, 0), (2, 0, 2), (3, 1, 1), (4, 2, 0), (6, 1, 2), (8, 0, 3), (9, 2, 1), (12, 2, 2), (15, 0, 4))
A_EVENTS = ((0, 3, 0), (1, 1, 3), (1, 3, 1), (2, 1, 4), (3, 3, 2), (3, 2, 3), (4, 2, 4), (5, 3, 3), (6, 3, 4))


def solution(mesh):
    side = math.isqrt(mesh.shape["sp"])

    def step(x, gain, wq, wk, wv, wo):
        own, depth = x.shape
        heads, kvh = wq.shape[1] // HEAD, wk.shape[1] // HEAD
        n = side * side
        place = lax.axis_index("sp") * own + jnp.arange(own)
        half = HEAD // 2
        angle = place.astype(jnp.float32)[:, None] * THETA ** (-jnp.arange(half, dtype=jnp.float32) / half)
        cos, sin = jnp.cos(angle), jnp.sin(angle)
        vmem, anywhere = pl.BlockSpec(memory_space=pltpu.VMEM), pl.BlockSpec(memory_space=pltpu.HBM)
        weights = 2 * (wq.size + wk.size + wv.size + wo.size)
        return pl.pallas_call(
            functools.partial(_kernel, side),
            out_shape=jax.ShapeDtypeStruct((own, depth), jnp.bfloat16),
            in_specs=[vmem] * 4 + [anywhere] * 4,
            out_specs=vmem,
            scratch_shapes=[
                pltpu.VMEM((own, depth), jnp.bfloat16),
                pltpu.VMEM((kvh, side, 2, side, own, HEAD), jnp.bfloat16),
                pltpu.VMEM((heads, own, HEAD), jnp.bfloat16),
                pltpu.VMEM((2 * heads // kvh, own, HEAD), jnp.bfloat16),
                pltpu.VMEM((depth // WIDE, own, WIDE), jnp.float32),
                pltpu.VMEM((SLOTS, depth, WIDE), jnp.bfloat16),
                pltpu.VMEM((n * own, STRIP * own), jnp.float32),
                pltpu.VMEM((n * own, STRIP * own), jnp.float32),
                pltpu.SemaphoreType.DMA((SLOTS,)),
                pltpu.SemaphoreType.DMA((kvh, 8)),
                pltpu.SemaphoreType.DMA((kvh, 8)),
            ],
            compiler_params=pltpu.CompilerParams(collective_id=0, has_side_effects=True, vmem_limit_bytes=67043328),
            cost_estimate=pl.CostEstimate(flops=own * weights + 4 * own * n * own * heads * HEAD, bytes_accessed=weights,
                                          transcendentals=own * n * own * heads),
        )(x, gain[None], jnp.concatenate([cos, cos], -1), jnp.concatenate([-sin, sin], -1), wq, wk, wv, wo)

    tokens, whole = P(("dp", "sp"), None), P(None, None)
    return jax.shard_map(
        step,
        mesh=mesh,
        in_specs=(tokens, P(None), whole, whole, whole, whole),
        out_specs=tokens,
        check_vma=False,
    )
```

```python
import functools
import math

import jax
import jax.numpy as jnp
from jax import lax
from jax.experimental import pallas as pl
from jax.experimental.pallas import tpu as pltpu
from jax.sharding import PartitionSpec as P

HEAD = 128
THETA = 10000
LOG2E = 1.4426950408889634
HIDDEN = -2e30
FAR = 1e30
WIDE = 512
SLOTS = 10
DEEP = 4
STRIP = 2


def _dot(a, b, ca=1, cb=0):
    return lax.dot_general(a, b, (((ca,), (cb,)), ((), ())), preferred_element_type=jnp.float32)


def _kernel(side, x_ref, gain_ref, cos_ref, sin_ref, wq_ref, wk_ref, wv_ref, wo_ref, y_ref,
            a_s, kv_s, q_s, o_s, acc_s, y_s, ring, s0, s1, cos_s, sin_s, ring_sem, y_sem, send_sem, recv_sem):
    own, depth = x_ref.shape
    heads, kvh = q_s.shape[0], kv_s.shape[0]
    group = heads // kvh
    pairs = kvh // 2
    n = side * side
    nq = heads * HEAD // WIDE
    per_q = WIDE // HEAD
    no = depth // WIDE
    rows_o = 2 * group * HEAD
    me = lax.axis_index("sp")
    mx, my = lax.div(me, side), lax.rem(me, side)

    q_end = [min(nq // 2, max(-(-nq * (h + 1) // (2 * kvh)), Q_END[h])) for h in range(kvh)] + [nq // 2]
    q_start = [0] + q_end[:-1]
    o_at = [next(h for h in range(kvh + 1) if O_END[h] > p) for p in range(pairs)]

    def pick(table, p):
        got = jnp.int32(table[-1])
        for i in range(len(table) - 2, -1, -1):
            got = jnp.where(p == i, table[i], got)
        return got

    chunks = pairs + nq + pairs * no
    runs = []
    for h in range(kvh + 1):
        for of_q, first, many in [(True, 2 * q_start[h], 2 * (q_end[h] - q_start[h]))] + [(False, p * no, no) for p in range(pairs) if o_at[p] == h]:
            if many and runs and runs[-1][0] == of_q:
                runs[-1] = (of_q, runs[-1][1], runs[-1][2] + many)
            elif many:
                runs.append((of_q, first, many))

    def issue(t):
        s = lax.rem(t, SLOTS)
        at = pairs

        def kv(p):
            cols = pl.ds(pl.multiple_of(p * (WIDE // 2), WIDE // 2), WIDE // 2)
            pltpu.make_async_copy(wk_ref.at[:, cols], ring.at[s, :, 0 : WIDE // 2], ring_sem.at[s]).start()
            pltpu.make_async_copy(wv_ref.at[:, cols], ring.at[s, :, WIDE // 2 :], ring_sem.at[s]).start()

        def q(c):
            pltpu.make_async_copy(wq_ref.at[:, pl.ds(pl.multiple_of(c * WIDE, WIDE), WIDE)], ring.at[s], ring_sem.at[s]).start()

        def o(p, c):
            pltpu.make_async_copy(
                wo_ref.at[pl.ds(pl.multiple_of(p * rows_o, rows_o), rows_o), pl.ds(pl.multiple_of(c * WIDE, WIDE), WIDE)],
                ring.at[s, 0:rows_o, :], ring_sem.at[s]).start()

        if isinstance(t, int) and t < pairs:
            kv(t)
            return
        is_q, is_o, qi, oi = False, False, jnp.int32(0), jnp.int32(0)
        for i, (of_q, first, many) in enumerate(runs):
            here = (t >= at) & (t < at + many)
            if of_q:
                is_q, qi = is_q | here, jnp.where(t >= at, t - (at - first), qi)
            else:
                is_o, oi = is_o | here, jnp.where(t >= at, t - (at - first), oi)
            at += many

        @pl.when(is_q)
        def _():
            q(qi)

        @pl.when(is_o)
        def _():
            o(lax.div(oi, no), lax.rem(oi, no))

    def landed(t, rows):
        s = lax.rem(t, SLOTS)
        ref = ring.at[s, 0:rows, :]
        pltpu.make_async_copy(ref, ref, ring_sem.at[s]).wait()
        return s

    def place(kind):
        return (mx, my) if kind == 0 else (my, mx)

    def device(kind, g, b):
        return g * side + b if kind == 0 else b * side + g

    def step(v, d):
        return lax.rem(v + d + side, side)

    def copy(ref, u, kind, i, peer):
        return pltpu.make_async_remote_copy(src_ref=ref, dst_ref=ref, send_sem=send_sem.at[u, kind, i], recv_sem=recv_sem.at[u, kind, i],
                                            device_id={"sp": peer}, device_id_type=pl.DeviceIdType.MESH)

    def transfers(u, kind):
        hs = pl.ds(*UNITS[u])
        g, b = place(kind)
        right1, left1 = device(kind, g, step(b, 1)), device(kind, g, step(b, -1))
        right2, left2 = device(kind, step(g, 1), b), device(kind, step(g, -1), b)
        blk = lambda dg, db: kv_s.at[hs, kind, step(g, dg), step(b, db)]
        part = lambda db, k: kv_s.at[hs, kind, g, step(b, db), pl.ds(k * (own // 2), own // 2)]
        half = lambda dg, k: kv_s.at[hs, kind, step(g, dg), pl.ds(k * (side // 2), side // 2)]
        sent = [(blk(0, 0), right1), (blk(0, 0), left1), (part(-1, 0), right1), (part(1, 1), left1)]
        come = [blk(0, -1), blk(0, 1), part(-2, 0), part(2, 1)]
        for d in (0, -1, 1, 2):
            sent += [(blk(0, d), right2), (blk(0, d), left2)]
            come += [blk(-1, d), blk(1, d)]
        sent += [(half(-1, 0), right2), (half(1, 1), left2)]
        come += [half(-2, 0), half(2, 1)]
        return sent, come

    def event(u, waits, starts):
        both = [transfers(u, kind) for kind in (0, 1)]
        for i in waits:
            for kind, (sent, come) in enumerate(both):
                copy(come[i], u, kind, i, me).wait_recv()
        for i in starts:
            for kind, (sent, come) in enumerate(both):
                copy(sent[i][0], u, kind, i, sent[i][1]).start()

    events = [((), (0, 1, 4, 5)), ((0, 1), (2, 3, 6, 7, 8, 9)), ((2, 3), (10, 11)), (tuple(range(4, 12)), (12, 13)), ((12, 13), ())]

    def happen(table, now):
        for at, *what in table:

            @pl.when(now == at)
            def _():
                for u, e in what:
                    event(u, *events[e])

    for t in range(min(SLOTS, chunks)):
        issue(t)

    barrier = pltpu.get_barrier_semaphore()
    around = [device(0, mx, step(my, 1)), device(0, mx, step(my, -1)), device(0, step(mx, 1), my), device(0, step(mx, -1), my)]
    for peer in around:
        pl.semaphore_signal(barrier, inc=1, device_id={"sp": peer}, device_id_type=pl.DeviceIdType.MESH)

    gain = jnp.concatenate([gain_ref[i : i + 1, :] for i in range(gain_ref.shape[0])], axis=1).astype(jnp.float32)
    cos_s[...] = jnp.concatenate([cos_ref[...], cos_ref[...]], axis=1)
    sin_s[...] = jnp.concatenate([-sin_ref[...], sin_ref[...]], axis=1)

    def norm(i, _):
        rows = pl.ds(pl.multiple_of(i * 16, 16), 16)
        wide = x_ref[rows, :].astype(jnp.float32)
        scale = lax.rsqrt(jnp.mean(wide * wide, -1, keepdims=True) + 1e-6)
        a_s[rows, :] = (wide * scale * gain).astype(jnp.bfloat16)

    lax.fori_loop(0, own // 16, norm, None)
    pl.semaphore_wait(barrier, len(around))

    def turned(t):
        wide = t.astype(jnp.bfloat16).astype(jnp.float32)
        return (wide * cos_s[...] + pltpu.roll(wide, HEAD // 2, 1) * sin_s[...]).astype(jnp.bfloat16)

    def kv_chunk(p, _):
        s = landed(p, depth)
        happen(KV_EVENTS, p)
        got = _dot(a_s[...], ring[s])
        issue(p + SLOTS)
        for j in (0, 1):
            k = turned(got[:, j * HEAD : (j + 1) * HEAD])
            v = got[:, WIDE // 2 + j * HEAD : WIDE // 2 + (j + 1) * HEAD]
            kv_s[2 * p + j, 0, mx, my] = k
            kv_s[2 * p + j, 1, my, mx] = v.T.astype(jnp.bfloat16)

    lax.fori_loop(0, pairs, kv_chunk, None)
    happen(((0, *KV_AFTER),), jnp.int32(0))
    for c in range(no):
        acc_s[c] = x_ref[:, c * WIDE : (c + 1) * WIDE].astype(jnp.float32)

    def q_chunks(i, t):
        slots = [landed(t + r, depth) for r in range(2)]
        got = [_dot(a_s[...], ring[s]).astype(jnp.bfloat16) for s in slots]
        for r in range(2):
            issue(t + r + SLOTS)
            for k in range(per_q):
                q_s[(2 * i + r) * per_q + k] = got[r][:, k * HEAD : (k + 1) * HEAD]
        happen(Q_EVENTS, i)
        return t + 2

    e = HEAD**-0.5 * LOG2E
    cols = STRIP * own
    shown = lax.broadcasted_iota(jnp.int32, (own, cols), 0) <= lax.rem(lax.broadcasted_iota(jnp.int32, (own, cols), 1), own)
    ones = jnp.ones((16, n * own), jnp.bfloat16)

    def attend(h):
        blocks = [lax.rem(me + i, n) for i in range(n)]
        hides = [None] + [jnp.where(at < me, 0.0, FAR) for at in blocks[1:]]
        blocks = [(lax.div(at, side), lax.rem(at, side)) for at in blocks]
        keys = jnp.concatenate([kv_s[h, 0, bx, by] for bx, by in blocks], axis=0)
        values = jnp.concatenate([jnp.concatenate([kv_s[h, 1, by, bx] for bx, by in blocks], axis=1), ones], axis=0)
        scores = (s0, s1)

        def score(i):
            q = jnp.concatenate([turned(q_s[h * group + i * STRIP + r]) for r in range(STRIP)], axis=0)
            top = None
            for r0 in range(0, n, 4):
                got = _dot(keys[r0 * own : (r0 + 4) * own], q, 1, 1)
                for r in range(r0, r0 + 4):
                    s = got[(r - r0) * own : (r - r0 + 1) * own, :]
                    if r == 0:
                        s = jnp.where(shown, s, HIDDEN)
                    scores[i % 2][r * own : (r + 1) * own, :] = s
                    part = s.reshape(own // 8, 8, cols).max(axis=0)
                    top = part if r == 0 else jnp.maximum(top, part - hides[r])
            return top

        def mix(i, top):
            s_ref = scores[i % 2]
            top = top.max(axis=0, keepdims=True)
            weights = [jnp.exp2((s_ref[r * own : (r + 1) * own, :] - (top if r == 0 else top + hides[r])) * e).astype(jnp.bfloat16) for r in range(n)]
            got = _dot(values, jnp.concatenate(weights, axis=0))
            out = (got[:HEAD] * (1 / got[HEAD : HEAD + 1])).T.astype(jnp.bfloat16)
            for r in range(STRIP):
                o_s[lax.rem(h, 4) * group + i * STRIP + r] = out[r * own : (r + 1) * own, :]

        strips = group // STRIP
        tops = [score(0)]
        for i in range(strips):
            if i + 1 < strips:
                tops.append(score(i + 1))
            mix(i, tops[i])

    def y_copy(c):
        return pltpu.make_async_copy(y_s.at[c], y_ref.at[:, pl.ds(pl.multiple_of(c * WIDE, WIDE), WIDE)], y_sem.at[c])

    def o_chunks(i, carry):
        t, p = carry
        slots = [landed(t + r, rows_o) for r in range(DEEP)]
        seen = jnp.concatenate([o_s[lax.rem(p, 2) * 2 * group + k] for k in range(2 * group)], axis=1)
        for r, s in enumerate(slots):
            acc_s[DEEP * i + r] += _dot(seen, ring[s, 0:rows_o, :])
        for r in range(DEEP):
            issue(t + r + SLOTS)

        @pl.when(p == pairs - 1)
        def _():
            for r in range(DEEP):
                y_s[DEEP * i + r] = acc_s[DEEP * i + r].astype(jnp.bfloat16)

            @pl.when(i > 0)
            def _():
                for r in range(DEEP):
                    y_copy(DEEP * i - DEEP + r).start()

        return t + DEEP, p

    def stage(h, t):
        t = lax.fori_loop(pick(q_start, h), pick(q_end, h), q_chunks, t)

        def project(p, t):
            return lax.fori_loop(0, no // DEEP, o_chunks, (t, p))[0]

        t = lax.fori_loop(pick([sum(at < k for at in o_at) for k in range(kvh + 1)], h),
                          pick([sum(at <= k for at in o_at) for k in range(kvh + 1)], h), project, t)
        happen(BEFORE, h)

        @pl.when(h < kvh)
        def _():
            attend(h)

        happen(AFTER, h)
        return t

    lax.fori_loop(0, kvh + 1, stage, jnp.int32(pairs))
    for u in range(len(UNITS)):
        for kind in (0, 1):
            for i, (ref, peer) in enumerate(transfers(u, kind)[0]):
                copy(ref, u, kind, i, peer).wait_send()
    for c in range(no - DEEP, no):
        y_copy(c).start()
    for c in range(no):
        y_copy(c).wait()


UNITS = ((0, 1), (1, 1), (2, 2), (4, 2), (6, 2))
Q_END = (4, 6, 10, 10, 12, 12, 12, 12)
O_END = (0, 0, 0, 0, 1, 2, 2, 3, 4)
KV_EVENTS = ((1, (0, 0), (1, 0)),)
KV_AFTER = ((0, 1),)
Q_EVENTS = ((0, (0, 2), (1, 1)), (1, (0, 3)), (2, (1, 2), (2, 0)), (3, (1, 3), (3, 0)), (5, (2, 2), (3, 1)), (6, (3, 2), (4, 0)),
            (10, (4, 2)))
BEFORE = ((0, (0, 4)), (1, (1, 4)), (2, (2, 4)), (4, (3, 4)), (6, (4, 4)))
AFTER = ((0, (2, 1)), (1, (2, 3)), (2, (3, 3), (4, 1)), (4, (4, 3)))


def solution(mesh):
    side = math.isqrt(mesh.shape["sp"])

    def step(x, gain, wq, wk, wv, wo):
        own, depth = x.shape
        heads, kvh = wq.shape[1] // HEAD, wk.shape[1] // HEAD
        n = side * side
        place = lax.axis_index("sp") * own + jnp.arange(own)
        half = HEAD // 2
        angle = place.astype(jnp.float32)[:, None] * THETA ** (-jnp.arange(half, dtype=jnp.float32) / half)
        cos, sin = jnp.cos(angle), jnp.sin(angle)
        vmem, anywhere = pl.BlockSpec(memory_space=pltpu.VMEM), pl.BlockSpec(memory_space=pltpu.HBM)
        weights = 2 * (wq.size + wk.size + wv.size + wo.size)
        return pl.pallas_call(
            functools.partial(_kernel, side),
            out_shape=jax.ShapeDtypeStruct((own, depth), jnp.bfloat16),
            in_specs=[vmem] * 4 + [anywhere] * 4,
            out_specs=anywhere,
            scratch_shapes=[
                pltpu.VMEM((own, depth), jnp.bfloat16),
                pltpu.VMEM((kvh, 2, side, side, own, HEAD), jnp.bfloat16),
                pltpu.VMEM((heads, own, HEAD), jnp.bfloat16),
                pltpu.VMEM((4 * heads // kvh, own, HEAD), jnp.bfloat16),
                pltpu.VMEM((depth // WIDE, own, WIDE), jnp.float32),
                pltpu.VMEM((depth // WIDE, own, WIDE), jnp.bfloat16),
                pltpu.VMEM((SLOTS, depth, WIDE), jnp.bfloat16),
                pltpu.VMEM((n * own, STRIP * own), jnp.float32),
                pltpu.VMEM((n * own, STRIP * own), jnp.float32),
                pltpu.VMEM((own, HEAD), jnp.float32),
                pltpu.VMEM((own, HEAD), jnp.float32),
                pltpu.SemaphoreType.DMA((SLOTS,)),
                pltpu.SemaphoreType.DMA((depth // WIDE,)),
                pltpu.SemaphoreType.DMA((len(UNITS), 2, 14)),
                pltpu.SemaphoreType.DMA((len(UNITS), 2, 14)),
            ],
            compiler_params=pltpu.CompilerParams(collective_id=0, has_side_effects=True, vmem_limit_bytes=67043328),
            cost_estimate=pl.CostEstimate(flops=own * weights + 4 * own * n * own * heads * HEAD, bytes_accessed=weights,
                                          transcendentals=own * n * own * heads),
        )(x, gain.reshape(-1, HEAD), cos, sin, wq, wk, wv, wo)

    tokens, whole = P(("dp", "sp"), None), P(None, None)
    return jax.shard_map(
        step,
        mesh=mesh,
        in_specs=(tokens, P(None), whole, whole, whole, whole),
        out_specs=tokens,
        check_vma=False,
    )
```

```python
import functools
import math

import jax
import jax.numpy as jnp
from jax import lax
from jax.experimental import pallas as pl
from jax.experimental.pallas import tpu as pltpu
from jax.sharding import PartitionSpec as P

HEAD = 128
THETA = 10000
LOG2E = 1.4426950408889634
HIDDEN = -2e30
FAR = 1e30
WIDE = 512
SLOTS = 10
DEEP = 4
STRIP = 2


def _dot(a, b, ca=1, cb=0):
    return lax.dot_general(a, b, (((ca,), (cb,)), ((), ())), preferred_element_type=jnp.float32)


def _kernel(side, x_ref, gain_ref, cos_ref, sin_ref, wq_ref, wk_ref, wv_ref, wo_ref, y_ref,
            a_s, kv_s, q_s, o_s, acc_s, y_s, ring, s0, s1, cos_s, sin_s, ring_sem, y_sem, send_sem, recv_sem):
    own, depth = x_ref.shape
    heads, kvh = q_s.shape[0], kv_s.shape[0]
    group = heads // kvh
    pairs = kvh // 2
    n = side * side
    nq = heads * HEAD // WIDE
    per_q = WIDE // HEAD
    no = depth // WIDE
    rows_o = 2 * group * HEAD
    me = lax.axis_index("sp")
    mx, my = lax.div(me, side), lax.rem(me, side)

    q_end = [min(nq // 2, max(-(-nq * (h + 1) // (2 * kvh)), Q_END[h])) for h in range(kvh)] + [nq // 2]
    q_start = [0] + q_end[:-1]
    o_at = [next(h for h in range(kvh + 1) if O_END[h] > p) for p in range(pairs)]

    def pick(table, p):
        got = jnp.int32(table[-1])
        for i in range(len(table) - 2, -1, -1):
            got = jnp.where(p == i, table[i], got)
        return got

    chunks = pairs + nq + pairs * no
    runs = []
    for h in range(kvh + 1):
        for of_q, first, many in [(True, 2 * q_start[h], 2 * (q_end[h] - q_start[h]))] + [(False, p * no, no) for p in range(pairs) if o_at[p] == h]:
            if many and runs and runs[-1][0] == of_q:
                runs[-1] = (of_q, runs[-1][1], runs[-1][2] + many)
            elif many:
                runs.append((of_q, first, many))

    def issue(t):
        s = lax.rem(t, SLOTS)
        at = pairs

        def kv(p):
            cols = pl.ds(pl.multiple_of(p * (WIDE // 2), WIDE // 2), WIDE // 2)
            pltpu.make_async_copy(wk_ref.at[:, cols], ring.at[s, :, 0 : WIDE // 2], ring_sem.at[s]).start()
            pltpu.make_async_copy(wv_ref.at[:, cols], ring.at[s, :, WIDE // 2 :], ring_sem.at[s]).start()

        def q(c):
            pltpu.make_async_copy(wq_ref.at[:, pl.ds(pl.multiple_of(c * WIDE, WIDE), WIDE)], ring.at[s], ring_sem.at[s]).start()

        def o(p, c):
            pltpu.make_async_copy(
                wo_ref.at[pl.ds(pl.multiple_of(p * rows_o, rows_o), rows_o), pl.ds(pl.multiple_of(c * WIDE, WIDE), WIDE)],
                ring.at[s, 0:rows_o, :], ring_sem.at[s]).start()

        if isinstance(t, int) and t < pairs:
            kv(t)
            return
        is_q, is_o, qi, oi = False, False, jnp.int32(0), jnp.int32(0)
        for i, (of_q, first, many) in enumerate(runs):
            here = (t >= at) & (t < at + many)
            if of_q:
                is_q, qi = is_q | here, jnp.where(t >= at, t - (at - first), qi)
            else:
                is_o, oi = is_o | here, jnp.where(t >= at, t - (at - first), oi)
            at += many

        @pl.when(is_q)
        def _():
            q(qi)

        @pl.when(is_o)
        def _():
            o(lax.div(oi, no), lax.rem(oi, no))

    def landed(t, rows):
        s = lax.rem(t, SLOTS)
        ref = ring.at[s, 0:rows, :]
        pltpu.make_async_copy(ref, ref, ring_sem.at[s]).wait()
        return s

    def place(kind):
        return (mx, my) if kind == 0 else (my, mx)

    def device(kind, g, b):
        return g * side + b if kind == 0 else b * side + g

    def step(v, d):
        return lax.rem(v + d + side, side)

    def copy(ref, u, kind, i, peer):
        return pltpu.make_async_remote_copy(src_ref=ref, dst_ref=ref, send_sem=send_sem.at[u, kind, i], recv_sem=recv_sem.at[u, kind, i],
                                            device_id={"sp": peer}, device_id_type=pl.DeviceIdType.MESH)

    def transfers(u, kind):
        hs = pl.ds(*UNITS[u])
        g, b = place(kind)
        right1, left1 = device(kind, g, step(b, 1)), device(kind, g, step(b, -1))
        right2, left2 = device(kind, step(g, 1), b), device(kind, step(g, -1), b)
        blk = lambda dg, db: kv_s.at[hs, kind, step(g, dg), step(b, db)]
        part = lambda db, k: kv_s.at[hs, kind, g, step(b, db), pl.ds(k * (own // 2), own // 2)]
        half = lambda dg, k: kv_s.at[hs, kind, step(g, dg), pl.ds(k * (side // 2), side // 2)]
        sent = [(blk(0, 0), right1), (blk(0, 0), left1), (part(-1, 0), right1), (part(1, 1), left1)]
        come = [blk(0, -1), blk(0, 1), part(-2, 0), part(2, 1)]
        for d in (0, -1, 1, 2):
            sent += [(blk(0, d), right2), (blk(0, d), left2)]
            come += [blk(-1, d), blk(1, d)]
        sent += [(half(-1, 0), right2), (half(1, 1), left2)]
        come += [half(-2, 0), half(2, 1)]
        return sent, come

    def event(u, waits, starts):
        both = [transfers(u, kind) for kind in (0, 1)]
        for i in waits:
            for kind, (sent, come) in enumerate(both):
                copy(come[i], u, kind, i, me).wait_recv()
        for i in starts:
            for kind, (sent, come) in enumerate(both):
                copy(sent[i][0], u, kind, i, sent[i][1]).start()

    events = [((), (0, 1, 4, 5)), ((0, 1), (2, 3, 6, 7, 8, 9)), ((2, 3), (10, 11)), (tuple(range(4, 12)), (12, 13)), ((12, 13), ())]

    def happen(table, now):
        for at, *what in table:

            @pl.when(now == at)
            def _():
                for u, e in what:
                    event(u, *events[e])

    for t in range(min(SLOTS, chunks)):
        issue(t)

    barrier = pltpu.get_barrier_semaphore()
    around = [device(0, mx, step(my, 1)), device(0, mx, step(my, -1)), device(0, step(mx, 1), my), device(0, step(mx, -1), my)]
    for peer in around:
        pl.semaphore_signal(barrier, inc=1, device_id={"sp": peer}, device_id_type=pl.DeviceIdType.MESH)

    gain = jnp.concatenate([gain_ref[i : i + 1, :] for i in range(gain_ref.shape[0])], axis=1).astype(jnp.float32)
    cos_s[...] = jnp.concatenate([cos_ref[...], cos_ref[...]], axis=1)
    sin_s[...] = jnp.concatenate([-sin_ref[...], sin_ref[...]], axis=1)

    def norm(i, _):
        rows = pl.ds(pl.multiple_of(i * 16, 16), 16)
        wide = x_ref[rows, :].astype(jnp.float32)
        scale = lax.rsqrt(jnp.mean(wide * wide, -1, keepdims=True) + 1e-6)
        a_s[rows, :] = (wide * scale * gain).astype(jnp.bfloat16)

    lax.fori_loop(0, own // 16, norm, None)
    pl.semaphore_wait(barrier, len(around))

    def turned(t):
        wide = t.astype(jnp.bfloat16).astype(jnp.float32)
        return (wide * cos_s[...] + pltpu.roll(wide, HEAD // 2, 1) * sin_s[...]).astype(jnp.bfloat16)

    def kv_chunk(p, _):
        s = landed(p, depth)
        happen(KV_EVENTS, p)
        got = _dot(a_s[...], ring[s])
        issue(p + SLOTS)
        for j in (0, 1):
            k = turned(got[:, j * HEAD : (j + 1) * HEAD])
            v = got[:, WIDE // 2 + j * HEAD : WIDE // 2 + (j + 1) * HEAD]
            kv_s[2 * p + j, 0, mx, my] = k
            kv_s[2 * p + j, 1, my, mx] = v.T.astype(jnp.bfloat16)

    lax.fori_loop(0, pairs, kv_chunk, None)
    happen(((0, *KV_AFTER),), jnp.int32(0))
    for c in range(no):
        acc_s[c] = x_ref[:, c * WIDE : (c + 1) * WIDE].astype(jnp.float32)

    def q_chunks(i, t):
        slots = [landed(t + r, depth) for r in range(2)]
        got = [_dot(a_s[...], ring[s]).astype(jnp.bfloat16) for s in slots]
        for r in range(2):
            issue(t + r + SLOTS)
            for k in range(per_q):
                q_s[(2 * i + r) * per_q + k] = got[r][:, k * HEAD : (k + 1) * HEAD]
        happen(Q_EVENTS, i)
        return t + 2

    e = HEAD**-0.5 * LOG2E
    cols = STRIP * own
    shown = lax.broadcasted_iota(jnp.int32, (own, cols), 0) <= lax.rem(lax.broadcasted_iota(jnp.int32, (own, cols), 1), own)
    ones = jnp.ones((16, n * own), jnp.bfloat16)

    def attend(h):
        blocks = [lax.rem(me + i, n) for i in range(n)]
        hides = [None] + [jnp.where(at < me, 0.0, FAR) for at in blocks[1:]]
        blocks = [(lax.div(at, side), lax.rem(at, side)) for at in blocks]
        keys = jnp.concatenate([kv_s[h, 0, bx, by] for bx, by in blocks], axis=0)
        values = jnp.concatenate([jnp.concatenate([kv_s[h, 1, by, bx] for bx, by in blocks], axis=1), ones], axis=0)
        scores = (s0, s1)

        def score(i):
            q = jnp.concatenate([turned(q_s[h * group + i * STRIP + r]) for r in range(STRIP)], axis=0)
            top = None
            for r0 in range(0, n, 8):
                got = _dot(keys[r0 * own : (r0 + 8) * own], q, 1, 1)
                for r in range(r0, r0 + 8):
                    s = got[(r - r0) * own : (r - r0 + 1) * own, :]
                    if r == 0:
                        s = jnp.where(shown, s, HIDDEN)
                    scores[i % 2][r * own : (r + 1) * own, :] = s
                    part = s.reshape(own // 8, 8, cols).max(axis=0)
                    top = part if r == 0 else jnp.maximum(top, part - hides[r])
            return top

        def mix(i, top):
            s_ref = scores[i % 2]
            top = top.max(axis=0, keepdims=True)
            weights = [jnp.exp2((s_ref[r * own : (r + 1) * own, :] - (top if r == 0 else top + hides[r])) * e).astype(jnp.bfloat16) for r in range(n)]
            got = _dot(values, jnp.concatenate(weights, axis=0))
            out = (got[:HEAD] * (1 / got[HEAD : HEAD + 1])).T.astype(jnp.bfloat16)
            for r in range(STRIP):
                o_s[lax.rem(h, 4) * group + i * STRIP + r] = out[r * own : (r + 1) * own, :]

        strips = group // STRIP
        tops = [score(0)]
        for i in range(strips):
            if i + 1 < strips:
                tops.append(score(i + 1))
            mix(i, tops[i])

    def y_copy(c):
        return pltpu.make_async_copy(y_s.at[c], y_ref.at[:, pl.ds(pl.multiple_of(c * WIDE, WIDE), WIDE)], y_sem.at[c])

    def o_chunks(i, carry):
        t, p = carry
        slots = [landed(t + r, rows_o) for r in range(DEEP)]
        seen = jnp.concatenate([o_s[lax.rem(p, 2) * 2 * group + k] for k in range(2 * group)], axis=1)
        for r, s in enumerate(slots):
            acc_s[DEEP * i + r] += _dot(seen, ring[s, 0:rows_o, :])
        for r in range(DEEP):
            issue(t + r + SLOTS)

        @pl.when(p == pairs - 1)
        def _():
            for r in range(DEEP):
                y_s[DEEP * i + r] = acc_s[DEEP * i + r].astype(jnp.bfloat16)

            @pl.when(i > 0)
            def _():
                for r in range(DEEP):
                    y_copy(DEEP * i - DEEP + r).start()

        return t + DEEP, p

    def stage(h, t):
        t = lax.fori_loop(pick(q_start, h), pick(q_end, h), q_chunks, t)

        def project(p, t):
            return lax.fori_loop(0, no // DEEP, o_chunks, (t, p))[0]

        t = lax.fori_loop(pick([sum(at < k for at in o_at) for k in range(kvh + 1)], h),
                          pick([sum(at <= k for at in o_at) for k in range(kvh + 1)], h), project, t)
        happen(BEFORE, h)

        @pl.when(h < kvh)
        def _():
            attend(h)

        happen(AFTER, h)
        return t

    lax.fori_loop(0, kvh + 1, stage, jnp.int32(pairs))
    for u in range(len(UNITS)):
        for kind in (0, 1):
            for i, (ref, peer) in enumerate(transfers(u, kind)[0]):
                copy(ref, u, kind, i, peer).wait_send()
    for c in range(no - DEEP, no):
        y_copy(c).start()
    for c in range(no):
        y_copy(c).wait()


UNITS = ((0, 1), (1, 1), (2, 2), (4, 2), (6, 2))
Q_END = (4, 7, 12, 12, 12, 12, 12, 12)
O_END = (0, 0, 0, 0, 1, 2, 3, 3, 4)
KV_EVENTS = ((1, (0, 0), (1, 0)),)
KV_AFTER = ((0, 1),)
Q_EVENTS = ((0, (0, 2), (1, 1)), (1, (0, 3)), (2, (1, 2), (2, 0)), (6, (2, 2), (3, 0)), (7, (2, 3)), (8, (3, 1)),
            (11, (3, 2), (4, 0)))
BEFORE = ((0, (0, 4)), (1, (1, 4)), (2, (2, 4)), (4, (3, 4), (4, 2)), (5, (4, 3)), (6, (4, 4)))
AFTER = ((0, (1, 3), (2, 1)), (2, (3, 3)), (3, (4, 1)))


def solution(mesh):
    side = math.isqrt(mesh.shape["sp"])

    def step(x, gain, wq, wk, wv, wo):
        own, depth = x.shape
        heads, kvh = wq.shape[1] // HEAD, wk.shape[1] // HEAD
        n = side * side
        place = lax.axis_index("sp") * own + jnp.arange(own)
        half = HEAD // 2
        angle = place.astype(jnp.float32)[:, None] * THETA ** (-jnp.arange(half, dtype=jnp.float32) / half)
        cos, sin = jnp.cos(angle), jnp.sin(angle)
        vmem, anywhere = pl.BlockSpec(memory_space=pltpu.VMEM), pl.BlockSpec(memory_space=pltpu.HBM)
        weights = 2 * (wq.size + wk.size + wv.size + wo.size)
        return pl.pallas_call(
            functools.partial(_kernel, side),
            out_shape=jax.ShapeDtypeStruct((own, depth), jnp.bfloat16),
            in_specs=[vmem] * 4 + [anywhere] * 4,
            out_specs=anywhere,
            scratch_shapes=[
                pltpu.VMEM((own, depth), jnp.bfloat16),
                pltpu.VMEM((kvh, 2, side, side, own, HEAD), jnp.bfloat16),
                pltpu.VMEM((heads, own, HEAD), jnp.bfloat16),
                pltpu.VMEM((4 * heads // kvh, own, HEAD), jnp.bfloat16),
                pltpu.VMEM((depth // WIDE, own, WIDE), jnp.float32),
                pltpu.VMEM((depth // WIDE, own, WIDE), jnp.bfloat16),
                pltpu.VMEM((SLOTS, depth, WIDE), jnp.bfloat16),
                pltpu.VMEM((n * own, STRIP * own), jnp.float32),
                pltpu.VMEM((n * own, STRIP * own), jnp.float32),
                pltpu.VMEM((own, HEAD), jnp.float32),
                pltpu.VMEM((own, HEAD), jnp.float32),
                pltpu.SemaphoreType.DMA((SLOTS,)),
                pltpu.SemaphoreType.DMA((depth // WIDE,)),
                pltpu.SemaphoreType.DMA((len(UNITS), 2, 14)),
                pltpu.SemaphoreType.DMA((len(UNITS), 2, 14)),
            ],
            compiler_params=pltpu.CompilerParams(collective_id=0, has_side_effects=True, vmem_limit_bytes=67043328),
            cost_estimate=pl.CostEstimate(flops=own * weights + 4 * own * n * own * heads * HEAD, bytes_accessed=weights,
                                          transcendentals=own * n * own * heads),
        )(x, gain.reshape(-1, HEAD), cos, sin, wq, wk, wv, wo)

    tokens, whole = P(("dp", "sp"), None), P(None, None)
    return jax.shard_map(
        step,
        mesh=mesh,
        in_specs=(tokens, P(None), whole, whole, whole, whole),
        out_specs=tokens,
        check_vma=False,
    )
```
